32 devices in a mesh: seq: 4 (over y, x), batch: 8 (over z, core).
Axes of the slice: x: 2, y: 2, z: 4, core: 2. Of those that a mesh axis runs over, the one named last changes fastest.
Arguments:
- attn_out: bfloat16 [16384, 2560], P(('seq', 'batch')), may hold values from -200 to 200
- out_grad: bfloat16 [16384, 2560], P(('seq', 'batch')), may hold values from -6 to 6
- master: float32 [2560, 2560], P(('seq', 'batch')), may hold values from -0.125 to 0.125
- moment_one: float32 [2560, 2560], P(('seq', 'batch')), may hold values from -4 to 4
- moment_two: float32 [2560, 2560], P(('seq', 'batch')), may hold values from 0.002 to 0.05
Outputs:
- input_grad: bfloat16 [16384, 2560], P(('seq', 'batch'))
- new_master: float32 [2560, 2560], P(('seq', 'batch'))
- new_moment_one: float32 [2560, 2560], P(('seq', 'batch'))
- new_moment_two: float32 [2560, 2560], P(('seq', 'batch'))
The draws below stay inside these ranges and needn't reach their ends.
All inputs are finite; a program needn't handle non-finite values.
Results may differ from the reference program's by a relative error of at most 0.01.
Values may be sent and summed in bfloat16 or wider, within the bound.
No kernel may reach another device: no remote copies, remote signals or barrier semaphores. Data moves between devices by JAX's collectives and lax.ppermute only.
A program may use at most 128 MiB of HBM per device.

```python
import math
import jax
import jax.numpy as jnp
from jax import lax

DIN = 2560
DOUT = 2560
TOK_DEV = 512
STEP = 10
TOKENS = 16384


def draw_attn_out(key, part):
    blocks = TOKENS // TOK_DEV
    feature_width = DIN // blocks
    first_key, second_key = jax.random.split(jax.random.fold_in(key, 11), 2)
    ramp = jnp.arange(DIN, dtype=jnp.float32) / jnp.float32(DIN)
    values = jax.random.normal(first_key, (TOKENS, DIN), jnp.float32)
    column = 10.0 ** ramp
    pairing = jax.random.permutation(second_key, blocks)
    token_block = jnp.arange(TOKENS) // TOK_DEV
    feature_block = jnp.arange(DIN) // feature_width
    spike = jnp.where(pairing[token_block][:, None] == feature_block[None, :], 6.0, 1.0)
    result = jnp.clip(values * column[None, :] * spike, -200.0, 200.0)
    return result.astype(jnp.bfloat16)


def steps_of(rng, shape, pieces, least, largest):
    factor_of, own = 1.0, jax.random.fold_in(rng, 6)
    for dim, parts in pieces:
        heights = jnp.exp(jax.random.uniform(jax.random.fold_in(own, dim), (parts,), jnp.float32, least / len(pieces), largest / len(pieces)))
        factor_of = factor_of * jnp.repeat(heights, shape[dim] // parts).reshape([-1 if axis == dim else 1 for axis in range(len(shape))])
    return factor_of


def noise(stream_key, extent, spread, most, shards=(), kind=jnp.bfloat16):
    drawn = jax.random.normal(stream_key, extent, jnp.float32) * spread
    if len(shards) > 0:
        drawn = steps_of(stream_key, extent, shards, -0.22, 0.18) * drawn
    return jnp.clip(drawn, min=-most, max=most).astype(kind)


def setup_inputs(seed: int = 0) -> dict:
    key_list = jax.random.split(jax.random.key(seed), 6)
    attn_out = draw_attn_out(jax.random.fold_in(key_list[5], 71), 0)
    out_grad = noise(key_list[1], (TOKENS, DOUT), 1.0, 6.0, ((0, 32),))
    master = noise(key_list[2], (DIN, DOUT), DIN ** -0.5, 0.125, ((0, 32),), jnp.float32)
    moment_one = noise(key_list[3], (DIN, DOUT), 0.3, 4.0, ((0, 32),), jnp.float32)
    moment_two = jnp.clip(jnp.exp(math.log(0.05) - 3.218876 * jax.random.uniform(key_list[4], (DIN, DOUT), jnp.float32) ** steps_of(key_list[4], (DIN, DOUT), ((0, 32),), -0.2, 0.2)), 0.002, 0.05)
    return dict(attn_out=attn_out, out_grad=out_grad, master=master, moment_one=moment_one, moment_two=moment_two)


def reference(attn_out, out_grad, master, moment_one, moment_two):
    weight = master.astype(jnp.bfloat16)
    input_grad = lax.dot_general(out_grad, weight, (((1,), (1,)), ((), ())), preferred_element_type=jnp.float32).astype(jnp.bfloat16)
    weight_grad = lax.dot_general(attn_out, out_grad, (((0,), (0,)), ((), ())), preferred_element_type=jnp.float32)
    grad_norm = jnp.sqrt(jnp.sum(weight_grad * weight_grad)) + 1e-06
    limit = jnp.sqrt(jnp.float32(DIN * DOUT))
    clipped = weight_grad * jnp.minimum(jnp.float32(1.0), limit / grad_norm)
    new_one = 0.9 * moment_one + 0.1 * clipped
    new_two = 0.999 * moment_two + 0.001 * clipped * clipped
    first_hat = new_one / (1.0 - 0.9 ** STEP)
    second_hat = new_two / (1.0 - 0.999 ** STEP)
    new_master = master - 0.01 * (first_hat / (jnp.sqrt(second_hat) + 1e-08) + 0.1 * master)
    return (input_grad, new_master, new_one, new_two)
```

```python
import functools

import jax
import jax.numpy as jnp
from jax import lax
from jax.experimental import pallas as pl
from jax.experimental.pallas import tpu as pltpu
from jax.sharding import PartitionSpec as P

STEP = 10
BF16 = jnp.bfloat16
F32 = jnp.float32
ALL = ("seq", "batch")


def adam(weight_grad, squares, master, moment_one, moment_two, size):
    grad_norm = jnp.sqrt(squares) + 1e-06
    limit = jnp.sqrt(jnp.float32(size))
    clipped = weight_grad * jnp.minimum(jnp.float32(1.0), limit / grad_norm)
    new_one = 0.9 * moment_one + 0.1 * clipped
    new_two = 0.999 * moment_two + 0.001 * clipped * clipped
    first_hat = new_one / (1.0 - 0.9**STEP)
    second_hat = new_two / (1.0 - 0.999**STEP)
    new_master = master - 0.01 * (first_hat / (jnp.sqrt(second_hat) + 1e-08) + 0.1 * master)
    return new_master, new_one, new_two


def native(attn_out, out_grad, master, moment_one, moment_two):
    weight = lax.all_gather(master.astype(BF16), ALL, axis=0, tiled=True)
    input_grad = lax.dot_general(
        out_grad, weight, (((1,), (1,)), ((), ())), preferred_element_type=F32
    ).astype(BF16)
    partial = lax.dot_general(
        attn_out, out_grad, (((0,), (0,)), ((), ())), preferred_element_type=F32
    ).astype(BF16)
    seq_summed = lax.psum_scatter(partial, "seq", scatter_dimension=0, tiled=True)
    weight_grad = lax.psum_scatter(seq_summed, "batch", scatter_dimension=0, tiled=True)
    weight_grad = weight_grad.astype(F32)
    squares = lax.psum(jnp.sum(weight_grad * weight_grad), ALL)
    size = attn_out.shape[1] * out_grad.shape[1]
    return (input_grad,) + adam(weight_grad, squares, master, moment_one, moment_two, size)


def wgrad_kernel(sel, attn_o, attn_p, og_o, og_p, out, turned):
    tok = attn_o.shape[0]

    @pl.when(pl.program_id(1) == 0)
    def _():
        turned[:, :tok] = attn_o[...].T
        turned[:, tok:] = attn_p[...].T

    out[...] = (
        jnp.dot(turned[:, :tok], og_o[...], preferred_element_type=F32)
        + jnp.dot(turned[:, tok:], og_p[...], preferred_element_type=F32)
    ).astype(out.dtype)


def wgrad(sel, attn_o, attn_p, out_grad, og_p, rows):
    tok, half = og_p.shape
    tile = 256 if half % 256 == 0 else 128
    tiles = half // tile
    return pl.pallas_call(
        wgrad_kernel,
        grid_spec=pltpu.PrefetchScalarGridSpec(
            num_scalar_prefetch=1,
            grid=(2, tiles),
            in_specs=[
                pl.BlockSpec((tok, rows), lambda i, j, s: (0, s[i])),
                pl.BlockSpec((tok, rows), lambda i, j, s: (0, s[i])),
                pl.BlockSpec((tok, tile), lambda i, j, s: (0, s[2] * tiles + j)),
                pl.BlockSpec((tok, tile), lambda i, j, s: (0, j)),
            ],
            out_specs=pl.BlockSpec((rows, tile), lambda i, j, s: (i, j)),
            scratch_shapes=[pltpu.VMEM((rows, 2 * tok), BF16)],
        ),
        out_shape=jax.ShapeDtypeStruct((2 * rows, half), BF16),
        compiler_params=pltpu.CompilerParams(vmem_limit_bytes=24 << 20),
        cost_estimate=pl.CostEstimate(
            flops=2 * 2 * rows * half * 2 * tok,
            bytes_accessed=2 * 2 * tok * (2 * rows + half) + 2 * 2 * rows * half,
            transcendentals=0,
        ),
    )(sel, attn_o, attn_p, out_grad, og_p)


def igrad_kernel(n_pieces, order, where, og, *refs):
    pieces, out = refs[:n_pieces], refs[n_pieces]
    weight, sems = refs[n_pieces + 1 :]
    groups, per = len(order), len(order[0])
    depth = pieces[0].shape[1]
    rows = weight.shape[1]

    copies = []
    for g in range(groups):
        for k, (piece, slot, row) in enumerate(order[g]):
            at = pl.multiple_of(where[groups + row], depth)
            copy = pltpu.make_async_copy(
                pieces[piece].at[slot], weight.at[g, pl.ds(at, depth)], sems.at[g, k]
            )
            copy.start()
            copies.append(copy)
    for g in range(groups):
        for k in range(per):
            copies[g * per + k].wait()
        lanes = pl.ds(pl.multiple_of(where[g] * rows, 128), rows)
        out[:, lanes] = lax.dot_general(
            og[...], weight[g], (((1,), (1,)), ((), ())), preferred_element_type=F32
        ).astype(out.dtype)


def igrad(where, og, pieces, order):
    tok, dout = og.shape
    depth = pieces[0].shape[1]
    groups, per = len(order), len(order[0])
    rows = per * depth
    return pl.pallas_call(
        functools.partial(igrad_kernel, len(pieces), order),
        in_specs=[
            pl.BlockSpec(memory_space=pltpu.SMEM),
            pl.BlockSpec(memory_space=pltpu.VMEM),
        ]
        + [pl.BlockSpec(memory_space=pl.ANY)] * len(pieces),
        out_specs=pl.BlockSpec(memory_space=pltpu.VMEM),
        out_shape=jax.ShapeDtypeStruct((tok, groups * rows), BF16),
        scratch_shapes=[
            pltpu.VMEM((groups, rows, dout), BF16),
            pltpu.SemaphoreType.DMA((groups, per)),
        ],
        compiler_params=pltpu.CompilerParams(vmem_limit_bytes=28 << 20),
        cost_estimate=pl.CostEstimate(
            flops=2 * tok * groups * rows * dout,
            bytes_accessed=2 * (2 * groups * rows * dout + 2 * tok * dout),
            transcendentals=0,
        ),
    )(where, og, *pieces)


def on_device(n_seq, n_batch, attn_out, out_grad, master, moment_one, moment_two):
    din, dout = attn_out.shape[1], out_grad.shape[1]
    half = dout // 2
    depth = master.shape[0]
    n_all = n_seq * n_batch
    n_line = n_all // 8
    chip_rows = 2 * depth
    rows = n_line * chip_rows
    me = lax.axis_index("seq") * n_batch + lax.axis_index("batch")
    core, chip = me % 2, me // 2
    line, place = chip // n_line, chip % n_line

    def perm(flip):
        return [(d, d ^ flip(d % 2)) for d in range(n_all)]

    top, low = n_all // 2, n_all // 4
    send = lambda a, flip: lax.ppermute(a, ALL, perm(flip))
    pair = lambda a: send(a, lambda c: 1)
    first = lambda a: send(a, lambda c: low if c else top)
    second = lambda a: send(a, lambda c: top if c else low)
    along = lambda a, m: send(a, lambda c: 2 * m)
    fmask = jnp.where(core == 0, 2, 1)
    smask = 3 - fmask

    own = master.astype(BF16)[None]
    unit = jnp.concatenate([own, second(own)], axis=0)
    attn_p = pair(attn_out)
    og_p = pair(lax.dynamic_slice_in_dim(out_grad, (1 - core) * half, half, axis=1))

    far = wgrad(jnp.stack([line ^ fmask, line ^ 3, core]), attn_out, attn_p, out_grad, og_p, rows)
    got_far = first(far)
    near = wgrad(jnp.stack([line, line ^ smask, core]), attn_out, attn_p, out_grad, og_p, rows)

    state = {0: unit}
    bit = n_line // 2
    while bit:
        state.update({m ^ bit: along(a, bit) for m, a in list(state.items())})
        bit //= 2
    over = {m: first(a) for m, a in state.items()}

    add = lambda *a: sum(v.astype(F32) for v in a)
    got_quarter = second(add(near[rows:], got_far[rows:]).astype(BF16))
    shape = (n_line, chip_rows, half)
    terms = [a.reshape(shape) for a in (near[:rows], got_far[:rows], got_quarter)]
    sums = {
        m: [lax.dynamic_index_in_dim(t, place ^ m, axis=0, keepdims=False) for t in terms]
        for m in range(n_line)
    }
    bit = 1
    while bit < n_line:
        for m in [m for m in sums if m & bit]:
            got = along(add(*sums.pop(m)).astype(BF16), bit)
            sums[m ^ bit].append(got)
        bit *= 2
    total = add(*sums[0]).reshape(2, depth, half)

    squares = jnp.broadcast_to(jnp.sum(total * total), (8, 128))
    bit = n_all // 2
    squares = squares + pair(squares)
    while bit > 1:
        squares = squares + send(squares, lambda c: bit)
        bit //= 2
    mine = lax.dynamic_index_in_dim(total, core, axis=0, keepdims=False)
    other = pair(lax.dynamic_index_in_dim(total, 1 - core, axis=0, keepdims=False))
    weight_grad = jnp.where(
        core == 0,
        jnp.concatenate([mine, other], axis=1),
        jnp.concatenate([other, mine], axis=1),
    )
    updated = adam(weight_grad, squares[0, 0], master, moment_one, moment_two, din * dout)

    pieces, order = [], [[], [], [], []]
    for m in state:
        for a, frame, over_first in (
            (state[m], 0, 0),
            (over[m], 0, 1),
            (pair(state[m]), 1, 0),
            (pair(over[m]), 1, 1),
        ):
            for slot in range(2):
                f, s = (over_first, slot) if frame == 0 else (slot, over_first)
                order[2 * f + s].append((len(pieces), slot, 2 * m + frame))
            pieces.append(a)
    groups = [line, line ^ smask, line ^ fmask, line ^ 3]
    offsets = []
    for m in range(n_line):
        for frame in range(2):
            offsets.append((place ^ m) * chip_rows + (core ^ frame) * depth)
    where = jnp.stack(groups + offsets).astype(jnp.int32)
    input_grad = igrad(where, out_grad, pieces, order)
    return (input_grad,) + updated


def solution(mesh):
    n_seq, n_batch = mesh.shape["seq"], mesh.shape["batch"]
    spec = P(ALL, None)

    def step(attn_out, out_grad, master, moment_one, moment_two):
        depth = master.shape[0] // (n_seq * n_batch)
        line_rows = master.shape[0] // 4
        fits = (
            n_seq % 4 == 0
            and n_batch % 2 == 0
            and (n_seq * n_batch) & (n_seq * n_batch - 1) == 0
            and depth % 16 == 0
            and line_rows % 128 == 0
            and out_grad.shape[1] % 256 == 0
        )
        body = functools.partial(on_device, n_seq, n_batch) if fits else native
        return jax.shard_map(
            body, mesh=mesh, in_specs=(spec,) * 5, out_specs=(spec,) * 4, check_vma=False
        )(attn_out, out_grad, master, moment_one, moment_two)

    return step
```
